32 devices in a mesh: grp: 2 (over y), ep: 4 (over x, core), hid: 4 (over z).
Axes of the slice: x: 2, y: 2, z: 4, core: 2. Of those that a mesh axis runs over, the one named last changes fastest.
Arguments:
- tokens: bfloat16 [1024, 4096], P(('grp', 'ep')), parts along dimension 0, may hold values from -6 to 6
- expert_ids: int32 [1024, 2], P(('grp', 'ep')), parts along dimension 0, may hold values from 0 to 3, all different within a row; in each aligned block of 128 rows (0 to 127, 128 to 255, ...) at most 64 rows name the same one
- gate_probs: float32 [1024, 2], P(('grp', 'ep')), parts along dimension 0, may hold values from 0.05 to 1
- w_gate: bfloat16 [16, 4096, 384], P(('ep', 'hid')), may hold values from -0.09375 to 0.09375
- w_up: bfloat16 [16, 4096, 384], P(('ep', 'hid')), may hold values from -0.09375 to 0.09375
- w_down: bfloat16 [16, 384, 4096], P(('ep', 'hid')), may hold values from -0.15625 to 0.15625
Outputs:
- mixed_out: bfloat16 [1024, 4096], P(('grp', 'ep'), 'hid'), parts along dimension 0
The draws below stay inside these ranges and needn't reach their ends.
There are 2 independent parts, one for each index of `grp`. The reference program is written for one: setup_inputs(seed, part) draws one part's arguments, and reference() takes and returns one part's arrays. A program takes and returns all parts, laid end to end along the dimension named above; an argument that names none is the same for every part. Nothing has to cross between parts.
Inputs may be any that keep to these rules, and one draw needn't show every extreme that they name: `expert_ids`: each token names 2 different experts. Among the 128 tokens of one index of ep (aligned blocks of rows) no expert is named by more than 64 tokens, and in every draw some expert is named by exactly 64 tokens of some block.
All inputs are finite; a program needn't handle non-finite values.
Results may differ from the reference program's by a relative error of at most 0.0085.
Values may be sent and summed in bfloat16 or wider, within the bound.
A program may use at most 128 MiB of HBM per device.

```python
import math
import jax
import jax.numpy as jnp
import numpy as np
from jax import lax

D = 4096
HIDDEN_SIZE = 1536
QUARTERS = 4
TOK_EP = 128
EXPERTS = 4
TOP = 2
CAP = 64
TOKENS = 512
N_EP = 4


def levels(own_key, dims, split, smallest, largest):
    def one(dim, blocks):
        steps = jax.random.uniform(jax.random.fold_in(jax.random.fold_in(own_key, 6), dim), (blocks,), jnp.float32, smallest / len(split), largest / len(split))
        return jnp.repeat(jnp.exp(steps), dims[dim] // blocks).reshape((-1,) + (1,) * (len(dims) - dim - 1))

    loudness = one(*split[0])
    for cut in split[1:]:
        loudness = loudness * one(*cut)
    return loudness


def shared_out(own_key, own, number, rows, count, top, most, lean):
    order = jax.random.permutation(own_key, count)
    crowded, common = shares(count, rows * top, most, lean, True), shares(count, rows * top, most, lean, False)
    places = jnp.arange(count)

    def named(tallies, turn):
        used = int((tallies > 0).sum())
        fixed = max(1, used // 4)
        passed = fixed + (places - fixed + turn * (used - fixed)) % max(1, count - fixed)
        return jnp.zeros((count,), jnp.int32).at[order[jnp.where(places < fixed, places, passed)]].set(jnp.asarray(tallies, jnp.int32))

    tallies = jnp.where(number % 4 == 0, named(crowded, number // 4), named(common, number - number // 4 - 1))
    mixed = jax.random.permutation(jax.random.fold_in(own, 3), count)
    donor, sink = mixed[0:count // 2 * 2:2], mixed[1:count // 2 * 2:2]
    room = jnp.minimum(tallies[donor] - 1, most - tallies[sink]) // 2
    room = jnp.where((donor == order[0]) | (sink == order[0]) | (tallies[sink] == 0), 0, jnp.maximum(room, 0))
    passed = jax.random.randint(jax.random.fold_in(own, 4), (count // 2,), 0, 1 << 20) % (room + 1)
    tallies = tallies.at[donor].add(-passed).at[sink].add(passed)
    items = jnp.searchsorted(jnp.cumsum(tallies), jnp.arange(rows * top), side="right").astype(jnp.int32)
    listing = items.reshape(top, rows).T
    listing = listing[jax.random.permutation(jax.random.fold_in(own, 1), rows)]
    turn = jax.random.randint(jax.random.fold_in(own, 2), (rows, 1), 0, top)
    return jnp.take_along_axis(listing, (jnp.arange(top)[None, :] + turn) % top, axis=1)


def shares(count, total, reach, slope, full):
    loads = [(1 << 20) // math.isqrt(standing ** slope) + 1 for standing in range(1, count + 1)]
    largest = reach if full else min(reach, max(-(-total // count), total * loads[0] // sum(loads)))
    least = 1 if total - largest >= count - 1 else 0
    given, rest = [largest] + [least] * (count - 1), total - largest - least * (count - 1)
    while rest > 0:
        movable = [i for i in range(1, count) if given[i] < largest] or [i for i in range(1, count) if given[i] < reach]
        pool, left = sum([loads[i] for i in movable]), rest
        for i in movable:
            extra = min(reach - given[i], max(1, left * loads[i] // pool), rest)
            given[i] = given[i] + extra
            rest = rest - extra
    return np.array(given)


def noise(own_key, extent, width, most, cuts=(), kind=jnp.bfloat16):
    array = width * jax.random.normal(own_key, extent, jnp.float32)
    if cuts:
        array = array * levels(own_key, extent, cuts, -0.22, 0.18)
    return jnp.clip(array, -most, most).astype(kind)


def setup_inputs(seed: int = 0, part: int = 0) -> dict:
    keys = jax.random.split(jax.random.key(seed), 7)
    part_keys = jax.random.split(jax.random.fold_in(keys[6], part), 7)
    tokens = noise(part_keys[0], (TOKENS, D), 1.0, 6.0, ((0, 4),))
    expert_ids_keys = jax.random.split(jax.random.fold_in(part_keys[1], 1), TOKENS // TOK_EP)
    expert_ids_turns = jax.random.permutation(jax.random.fold_in(part_keys[1], 3), TOKENS // TOK_EP)
    expert_ids = jax.vmap(lambda own, number: shared_out(jax.random.fold_in(part_keys[1], 2), own, number, TOK_EP, EXPERTS, TOP, CAP, 2))(expert_ids_keys, expert_ids_turns).reshape((TOKENS, TOP))
    gate_probs = jnp.clip(jnp.exp(math.log(1.0) - 2.9957323 * jax.random.uniform(part_keys[2], (TOKENS, TOP), jnp.float32) ** levels(part_keys[2], (TOKENS, TOP), ((0, 4),), -0.2, 0.2)), 0.05, 1.0)
    w_gate = noise(keys[3], (EXPERTS * QUARTERS, D, HIDDEN_SIZE // QUARTERS), D ** -0.5, 0.09375, ((0, 16),))
    w_up = noise(keys[4], (EXPERTS * QUARTERS, D, HIDDEN_SIZE // QUARTERS), D ** -0.5, 0.09375, ((0, 16),))
    w_down = noise(keys[5], (EXPERTS * QUARTERS, HIDDEN_SIZE // QUARTERS, D), HIDDEN_SIZE ** -0.5, 0.15625, ((0, 16),))
    return {"tokens": tokens, "expert_ids": expert_ids, "gate_probs": gate_probs, "w_gate": w_gate, "w_up": w_up, "w_down": w_down}


def reference(tokens, expert_ids, gate_probs, w_gate, w_up, w_down):
    tok_total, model_width = tokens.shape
    pick_count = expert_ids.shape[1]
    experts = w_gate.shape[0] // QUARTERS
    quarter_width = w_gate.shape[2]
    slots_each = N_EP * CAP
    grouped = expert_ids.reshape(N_EP, TOK_EP * pick_count)
    onehot = (grouped[:, :, None] == jnp.arange(experts, dtype=jnp.int32)[None, None, :]).astype(jnp.int32)
    before = jnp.cumsum(onehot, axis=1) - onehot
    position = jnp.sum(before * onehot, axis=2).astype(jnp.int32)
    block_index = jnp.arange(N_EP, dtype=jnp.int32)[:, None]
    slot_index = (grouped * slots_each + block_index * CAP + position).reshape(-1).astype(jnp.int32)
    routed_rows = jnp.repeat(tokens, pick_count, axis=0)
    buffer = jnp.zeros((experts * slots_each, model_width), tokens.dtype)
    buffer = buffer.at[slot_index].set(routed_rows).reshape(experts, slots_each, model_width)
    gate_stack = w_gate.reshape(experts, QUARTERS, model_width, quarter_width)
    up_stack = w_up.reshape(experts, QUARTERS, model_width, quarter_width)
    down_stack = w_down.reshape(experts, QUARTERS, quarter_width, model_width)

    def expert_fn(operands):
        expert_rows, gate_matrix, up_matrix, down_matrix = operands
        running = jnp.zeros((expert_rows.shape[0], model_width), jnp.float32)
        for index in range(QUARTERS):
            gate_act = jnp.dot(expert_rows, gate_matrix[index], preferred_element_type=jnp.float32)
            up_act = jnp.dot(expert_rows, up_matrix[index], preferred_element_type=jnp.float32)
            hidden = (jax.nn.silu(gate_act) * up_act).astype(jnp.bfloat16)
            piece_sum = jnp.dot(hidden, down_matrix[index], preferred_element_type=jnp.float32).astype(jnp.bfloat16)
            running = running + lax.optimization_barrier(piece_sum).astype(jnp.float32)
        return running

    outputs = lax.map(expert_fn, (buffer, gate_stack, up_stack, down_stack))
    picked = outputs.reshape(-1, model_width)[slot_index].reshape(tok_total, pick_count, model_width)
    weights = lax.optimization_barrier(gate_probs.astype(jnp.bfloat16)).astype(jnp.float32)
    mixed_out = jnp.einsum('tk,tkd->td', weights, picked, precision=lax.Precision.HIGHEST)
    return mixed_out.astype(jnp.bfloat16)
```

```python
import functools

import jax
import jax.numpy as jnp
from jax import lax
from jax.experimental import pallas as pl
from jax.experimental.pallas import tpu as pltpu
from jax.sharding import PartitionSpec as P

QUARTERS = 4
ROW_CHUNKS = 2
RETURN_CHUNKS = 4
MESH = pl.DeviceIdType.MESH
F32 = jnp.float32
BF16 = jnp.bfloat16


def kernel(ep_count, hid_count, tokens, ids, probs, w_gate, w_up, w_down, out,
           gate_buf, up_buf, down_buf, key_t, combine, outgoing, sibling_out, slots, hidden,
           partial, returned, owner_out, owner_in,
           weight_sem, disp_send, disp_recv, fwd_send, fwd_recv, ret_send, ret_recv, sum_send, sum_recv):
    ep = lax.axis_index("ep")
    hid = lax.axis_index("hid")
    groups = hid_count // QUARTERS
    group = hid // QUARTERS
    rows, width = tokens.shape
    picks = ids.shape[1]
    cap = slots.shape[1]
    half = width // 2
    pairs = ep_count // 2
    pair = ep // 2
    core = ep % 2
    sibling = pair * 2 + 1 - core
    mate = hid + 1 - 2 * (hid % 2)
    my_half = pl.ds(pl.multiple_of((hid % 2) * half, half), half)
    piece = cap // ROW_CHUNKS
    feat = width // hid_count
    chunks = partial.shape[0]
    step = feat // chunks

    loads = [pltpu.make_async_copy(src.at[0], dst, weight_sem.at[i])
             for i, (src, dst) in enumerate(((w_gate, gate_buf), (w_up, up_buf), (w_down, down_buf)))]
    for load in loads:
        load.start()

    barrier = pltpu.get_barrier_semaphore()
    for off in range(1, ep_count):
        pl.semaphore_signal(barrier, 1, device_id={"ep": lax.rem(ep + off, ep_count)}, device_id_type=MESH)
    for off in range(1, hid_count):
        pl.semaphore_signal(barrier, 1, device_id={"hid": lax.rem(hid + off, hid_count)}, device_id_type=MESH)

    lane = lax.broadcasted_iota(jnp.int32, (rows, 128), 1) * groups + group
    count = jnp.zeros((rows, 128), F32)
    weight = jnp.zeros((rows, 128), F32)
    gate_round = probs[...].astype(BF16).astype(F32)
    for k in range(picks):
        hit = ids[:, k:k + 1] == lane
        count = jnp.where(hit, 1.0, count)
        weight = jnp.where(hit, gate_round[:, k:k + 1], weight)
    earlier = (lax.broadcasted_iota(jnp.int32, (rows, rows), 1)
               < lax.broadcasted_iota(jnp.int32, (rows, rows), 0)).astype(F32).astype(BF16)
    before = jnp.dot(earlier, count.astype(BF16), preferred_element_type=F32)
    key = jnp.where(count > 0.5, before, -1000.0).astype(jnp.int32)
    key_t[...] = jnp.where(count > 0.5, before, -1000.0).T.astype(jnp.int32)

    def pick_rows(first, blocks):
        row = lax.broadcasted_iota(jnp.int32, (cap, rows), 0)
        parts = [(key_t[pl.ds(first + b, 1), :] == row).astype(F32).astype(BF16) for b in range(blocks)]
        return jnp.concatenate(parts, axis=0) if blocks > 1 else parts[0]

    tile = min(half, 512)
    sends = []
    for off in range(1, pairs):
        other = lax.rem(pair + off, pairs)
        chosen = pick_rows(2 * other, 2)
        for col in range(0, half, tile):
            src = pl.ds(pl.multiple_of((hid % 2) * half + col, tile), tile)
            rows_out = jnp.dot(chosen, tokens[:, src], preferred_element_type=F32).astype(BF16)
            outgoing[off - 1, :, :, col:col + tile] = rows_out.reshape(2, cap, tile)
    pl.semaphore_wait(barrier, ep_count - 1 + hid_count - 1)
    for off in range(1, pairs):
        other = lax.rem(pair + off, pairs)
        for r in range(ROW_CHUNKS):
            part = pl.ds(r * piece, piece)
            for flip in range(2):
                who = core if flip == 0 else 1 - core
                copy = pltpu.make_async_remote_copy(
                    src_ref=outgoing.at[off - 1, who, part],
                    dst_ref=slots.at[ep, part, my_half],
                    send_sem=disp_send.at[off, r, flip],
                    recv_sem=disp_recv.at[ep, r],
                    device_id={"ep": 2 * other + who}, device_id_type=MESH)
                copy.start()
                sends.append(copy)

    for col in range(0, width, tile):
        sibling_out[:, col:col + tile] = jnp.dot(
            pick_rows(sibling, 1), tokens[:, col:col + tile], preferred_element_type=F32).astype(BF16)
    to_sibling = pltpu.make_async_remote_copy(
        src_ref=sibling_out, dst_ref=slots.at[ep],
        send_sem=disp_send.at[0, 0, 0], recv_sem=disp_recv.at[ep, 0],
        device_id={"ep": sibling}, device_id_type=MESH)
    to_sibling.start()
    sends.append(to_sibling)
    for col in range(0, width, tile):
        slots[ep, :, col:col + tile] = jnp.dot(
            pick_rows(ep, 1), tokens[:, col:col + tile], preferred_element_type=F32).astype(BF16)

    lanes = lax.broadcasted_iota(jnp.int32, (rows, cap), 1)
    for b in range(ep_count):
        combine[:, b * cap:(b + 1) * cap] = jnp.where(
            key[:, b:b + 1] == lanes, weight[:, b:b + 1], 0.0).astype(BF16)

    def act(which):
        block = slots[pl.ds(2 * which, 2)].reshape(2 * cap, width)
        gate_act = jnp.dot(block, gate_buf[...], preferred_element_type=F32)
        up_act = jnp.dot(block, up_buf[...], preferred_element_type=F32)
        value = gate_act / (1.0 + jnp.exp(-gate_act)) * up_act
        hidden[pl.ds(pl.multiple_of(which * 2 * cap, 2 * cap), 2 * cap), :] = value.astype(BF16)

    pltpu.make_async_remote_copy(
        src_ref=sibling_out, dst_ref=slots.at[sibling],
        send_sem=disp_send.at[0, 0, 0], recv_sem=disp_recv.at[sibling, 0],
        device_id={"ep": sibling}, device_id_type=MESH).wait_recv()
    loads[0].wait()
    loads[1].wait()
    act(pair)

    forwards = []
    for off in range(1, pairs):
        other = lax.rem(pair + pairs - off, pairs)
        for r in range(ROW_CHUNKS):
            part = pl.ds(r * piece, piece)
            for flip in range(2):
                source = 2 * other + (core if flip == 0 else 1 - core)
                landed = slots.at[source, part, my_half]
                pltpu.make_async_remote_copy(
                    src_ref=landed, dst_ref=landed,
                    send_sem=disp_send.at[off, r, flip], recv_sem=disp_recv.at[source, r],
                    device_id={"ep": source}, device_id_type=MESH).wait_recv()
                copy = pltpu.make_async_remote_copy(
                    src_ref=landed, dst_ref=landed,
                    send_sem=fwd_send.at[off, r, flip], recv_sem=fwd_recv.at[off, r, flip],
                    device_id={"hid": mate}, device_id_type=MESH)
                copy.start()
                forwards.append(copy)
    per = 2 * ROW_CHUNKS
    for off in range(1, pairs):
        for copy in forwards[(off - 1) * per:off * per]:
            copy.wait_recv()
        act(lax.rem(pair + pairs - off, pairs))

    loads[2].wait()
    for c in range(chunks):
        for h in range(hid_count):
            col = h * feat + c * step
            value = jnp.dot(hidden[...], down_buf[:, col:col + step], preferred_element_type=F32)
            partial[c, :, :, h * step:(h + 1) * step] = value.astype(BF16).reshape(ep_count, cap, step)
        for off in list(range(2, ep_count)) + [1]:
            owner = lax.rem(ep + off, ep_count)
            copy = pltpu.make_async_remote_copy(
                src_ref=partial.at[c, owner], dst_ref=returned.at[c, ep],
                send_sem=ret_send.at[c, off], recv_sem=ret_recv.at[c, ep],
                device_id={"ep": owner}, device_id_type=MESH)
            copy.start()
            sends.append(copy)
        returned[c, ep] = partial[c, ep]

    for c in range(chunks):
        for off in range(1, ep_count):
            source = lax.rem(ep + off, ep_count)
            pltpu.make_async_remote_copy(
                src_ref=partial.at[c, source], dst_ref=returned.at[c, source],
                send_sem=ret_send.at[c, off], recv_sem=ret_recv.at[c, source],
                device_id={"ep": source}, device_id_type=MESH).wait_recv()
        for h in range(hid_count):
            block = returned[c, :, :, h * step:(h + 1) * step].reshape(ep_count * cap, step)
            owner_out[c, h] = jnp.dot(combine[...], block, preferred_element_type=F32).astype(BF16)
        for off in list(range(2, hid_count)) + [1]:
            target = lax.rem(hid + off, hid_count)
            copy = pltpu.make_async_remote_copy(
                src_ref=owner_out.at[c, target], dst_ref=owner_in.at[c, hid],
                send_sem=sum_send.at[c, off], recv_sem=sum_recv.at[c, hid],
                device_id={"hid": target}, device_id_type=MESH)
            copy.start()
            sends.append(copy)

    for c in range(chunks):
        total = owner_out[c, hid].astype(F32)
        for off in range(1, hid_count):
            source = lax.rem(hid + off, hid_count)
            pltpu.make_async_remote_copy(
                src_ref=owner_out.at[c, source], dst_ref=owner_in.at[c, source],
                send_sem=sum_send.at[c, off], recv_sem=sum_recv.at[c, source],
                device_id={"hid": source}, device_id_type=MESH).wait_recv()
            total = total + owner_in[c, source].astype(F32)
        out[:, c * step:(c + 1) * step] = total.astype(BF16)
    for copy in sends + forwards:
        copy.wait_send()


def local(ep_count, hid_count, tokens, expert_ids, gate_probs, w_gate, w_up, w_down):
    rows, width = tokens.shape
    inner = w_gate.shape[2]
    cap = rows // 2
    feat = width // hid_count
    chunks = RETURN_CHUNKS
    step = feat // chunks
    others = max(ep_count // 2 - 1, 1)
    vmem = pl.BlockSpec(memory_space=pltpu.VMEM)
    hbm = pl.BlockSpec(memory_space=pl.ANY)
    dma = pltpu.SemaphoreType.DMA
    return pl.pallas_call(
        functools.partial(kernel, ep_count, hid_count),
        out_shape=jax.ShapeDtypeStruct((rows, feat), BF16),
        in_specs=[vmem, vmem, vmem, hbm, hbm, hbm],
        out_specs=vmem,
        scratch_shapes=[
            pltpu.VMEM((width, inner), BF16),
            pltpu.VMEM((width, inner), BF16),
            pltpu.VMEM((inner, width), BF16),
            pltpu.VMEM((128, rows), jnp.int32),
            pltpu.VMEM((rows, ep_count * cap), BF16),
            pltpu.VMEM((others, 2, cap, width // 2), BF16),
            pltpu.VMEM((cap, width), BF16),
            pltpu.VMEM((ep_count, cap, width), BF16),
            pltpu.VMEM((ep_count * cap, inner), BF16),
            pltpu.VMEM((chunks, ep_count, cap, hid_count * step), BF16),
            pltpu.VMEM((chunks, ep_count, cap, hid_count * step), BF16),
            pltpu.VMEM((chunks, hid_count, rows, step), BF16),
            pltpu.VMEM((chunks, hid_count, rows, step), BF16),
            dma((3,)),
            dma((ep_count // 2, ROW_CHUNKS, 2)),
            dma((ep_count, ROW_CHUNKS)),
            dma((ep_count // 2, ROW_CHUNKS, 2)),
            dma((ep_count // 2, ROW_CHUNKS, 2)),
            dma((chunks, ep_count)),
            dma((chunks, ep_count)),
            dma((chunks, hid_count)),
            dma((chunks, hid_count)),
        ],
        compiler_params=pltpu.CompilerParams(
            collective_id=0, has_side_effects=True, vmem_limit_bytes=60 * 2**20),
    )(tokens, expert_ids, gate_probs, w_gate, w_up, w_down)


def solution(mesh):
    in_specs = (
        P(("grp", "ep"), None),
        P(("grp", "ep"), None),
        P(("grp", "ep"), None),
        P(("ep", "hid"), None, None),
        P(("ep", "hid"), None, None),
        P(("ep", "hid"), None, None),
    )
    out_specs = P(("grp", "ep"), "hid")
    body = functools.partial(local, mesh.shape["ep"], mesh.shape["hid"])
    return jax.shard_map(body, mesh=mesh, in_specs=in_specs, out_specs=out_specs, check_vma=False)
```

```python
import functools

import jax
import jax.numpy as jnp
from jax import lax
from jax.experimental import pallas as pl
from jax.experimental.pallas import tpu as pltpu
from jax.sharding import PartitionSpec as P

QUARTERS = 4
ROW_CHUNKS = 4
RETURN_STEP = 128
MESH = pl.DeviceIdType.MESH
F32 = jnp.float32
BF16 = jnp.bfloat16


def kernel(ep_count, hid_count, tokens, ids, probs, w_gate, w_up, w_down, out,
           gate_buf, up_buf, down_buf, key_t, combine, outgoing, sibling_out, slots, hidden,
           partial, returned, owner_out, owner_in,
           weight_sem, disp_send, disp_recv, fwd_send, fwd_recv, ret_send, ret_recv, sum_send, sum_recv):
    ep = lax.axis_index("ep")
    hid = lax.axis_index("hid")
    groups = hid_count // QUARTERS
    group = hid // QUARTERS
    rows, width = tokens.shape
    picks = ids.shape[0]
    cap = slots.shape[1]
    half = width // 2
    pairs = ep_count // 2
    pair = ep // 2
    core = ep % 2
    sibling = pair * 2 + 1 - core
    mate = hid + 1 - 2 * (hid % 2)
    my_half = pl.ds(pl.multiple_of((hid % 2) * half, half), half)
    piece = cap // ROW_CHUNKS
    feat = width // hid_count
    chunks = partial.shape[0]
    step = feat // chunks

    loads = [pltpu.make_async_copy(src.at[0], dst, weight_sem.at[i])
             for i, (src, dst) in enumerate(((w_gate, gate_buf), (w_up, up_buf), (w_down, down_buf)))]
    for load in loads:
        load.start()

    barrier = pltpu.get_barrier_semaphore()
    for off in range(1, ep_count):
        pl.semaphore_signal(barrier, 1, device_id={"ep": lax.rem(ep + off, ep_count)}, device_id_type=MESH)
    for off in range(1, hid_count):
        pl.semaphore_signal(barrier, 1, device_id={"hid": lax.rem(hid + off, hid_count)}, device_id_type=MESH)

    name = lax.broadcasted_iota(jnp.int32, (128, rows), 0) * groups + group
    count = jnp.zeros((128, rows), F32)
    weight = jnp.zeros((128, rows), F32)
    gate_round = probs[...].astype(BF16).astype(F32)
    for k in range(picks):
        hit = ids[k:k + 1, :] == name
        count = jnp.where(hit, 1.0, count)
        weight = jnp.where(hit, gate_round[k:k + 1, :], weight)
    earlier = (lax.broadcasted_iota(jnp.int32, (rows, rows), 0)
               < lax.broadcasted_iota(jnp.int32, (rows, rows), 1)).astype(F32).astype(BF16)
    before = jnp.dot(count.astype(BF16), earlier, preferred_element_type=F32)
    place = jnp.where(count > 0.5, before, -1000.0)
    key_t[...] = place.astype(jnp.int32)

    def pick_rows(first, blocks):
        row = lax.broadcasted_iota(jnp.int32, (cap, rows), 0)
        parts = [(key_t[pl.ds(first + b, 1), :] == row).astype(F32).astype(BF16) for b in range(blocks)]
        return jnp.concatenate(parts, axis=0) if blocks > 1 else parts[0]

    tile = min(half, 512)
    sends = []
    for off in range(1, pairs):
        other = lax.rem(pair + off, pairs)
        chosen = pick_rows(2 * other, 2)
        for col in range(0, half, tile):
            src = pl.ds(pl.multiple_of((hid % 2) * half + col, tile), tile)
            rows_out = jnp.dot(chosen, tokens[:, src], preferred_element_type=F32).astype(BF16)
            outgoing[off - 1, :, :, col:col + tile] = rows_out.reshape(2, cap, tile)
    pl.semaphore_wait(barrier, ep_count - 1 + hid_count - 1)
    for off in range(1, pairs):
        other = lax.rem(pair + off, pairs)
        for r in range(ROW_CHUNKS):
            part = pl.ds(r * piece, piece)
            for flip in range(2):
                who = core if flip == 0 else 1 - core
                copy = pltpu.make_async_remote_copy(
                    src_ref=outgoing.at[off - 1, who, part],
                    dst_ref=slots.at[ep, part, my_half],
                    send_sem=disp_send.at[off, r, flip],
                    recv_sem=disp_recv.at[ep, r],
                    device_id={"ep": 2 * other + who}, device_id_type=MESH)
                copy.start()
                sends.append(copy)

    for col in range(0, width, tile):
        sibling_out[:, col:col + tile] = jnp.dot(
            pick_rows(sibling, 1), tokens[:, col:col + tile], preferred_element_type=F32).astype(BF16)
    to_sibling = pltpu.make_async_remote_copy(
        src_ref=sibling_out, dst_ref=slots.at[ep],
        send_sem=disp_send.at[0, 0, 0], recv_sem=disp_recv.at[ep, 0],
        device_id={"ep": sibling}, device_id_type=MESH)
    to_sibling.start()
    sends.append(to_sibling)
    for col in range(0, width, tile):
        slots[ep, :, col:col + tile] = jnp.dot(
            pick_rows(ep, 1), tokens[:, col:col + tile], preferred_element_type=F32).astype(BF16)

    lanes = lax.broadcasted_iota(jnp.int32, (rows, cap), 1)
    key = place.T.astype(jnp.int32)
    weight = weight.T
    for b in range(ep_count):
        combine[:, b * cap:(b + 1) * cap] = jnp.where(
            key[:, b:b + 1] == lanes, weight[:, b:b + 1], 0.0).astype(BF16)

    def act(which):
        block = slots[pl.ds(2 * which, 2)].reshape(2 * cap, width)
        gate_act = jnp.dot(block, gate_buf[...], preferred_element_type=F32)
        up_act = jnp.dot(block, up_buf[...], preferred_element_type=F32)
        value = gate_act / (1.0 + jnp.exp(-gate_act)) * up_act
        hidden[pl.ds(pl.multiple_of(which * 2 * cap, 2 * cap), 2 * cap), :] = value.astype(BF16)

    pltpu.make_async_remote_copy(
        src_ref=sibling_out, dst_ref=slots.at[sibling],
        send_sem=disp_send.at[0, 0, 0], recv_sem=disp_recv.at[sibling, 0],
        device_id={"ep": sibling}, device_id_type=MESH).wait_recv()
    loads[0].wait()
    loads[1].wait()
    act(pair)

    forwards = []
    for off in range(1, pairs):
        other = lax.rem(pair + pairs - off, pairs)
        for r in range(ROW_CHUNKS):
            part = pl.ds(r * piece, piece)
            for flip in range(2):
                source = 2 * other + (core if flip == 0 else 1 - core)
                landed = slots.at[source, part, my_half]
                pltpu.make_async_remote_copy(
                    src_ref=landed, dst_ref=landed,
                    send_sem=disp_send.at[off, r, flip], recv_sem=disp_recv.at[source, r],
                    device_id={"ep": source}, device_id_type=MESH).wait_recv()
                copy = pltpu.make_async_remote_copy(
                    src_ref=landed, dst_ref=landed,
                    send_sem=fwd_send.at[off, r, flip], recv_sem=fwd_recv.at[off, r, flip],
                    device_id={"hid": mate}, device_id_type=MESH)
                copy.start()
                forwards.append(copy)
    per = 2 * ROW_CHUNKS
    for off in range(1, pairs):
        for copy in forwards[(off - 1) * per:off * per]:
            copy.wait_recv()
        act(lax.rem(pair + pairs - off, pairs))

    loads[2].wait()
    for c in range(chunks):
        for h in range(hid_count):
            col = h * feat + c * step
            value = jnp.dot(hidden[...], down_buf[:, col:col + step], preferred_element_type=F32)
            partial[c, :, :, h * step:(h + 1) * step] = value.astype(BF16).reshape(ep_count, cap, step)
        for off in list(range(2, ep_count)) + [1]:
            owner = lax.rem(ep + off, ep_count)
            copy = pltpu.make_async_remote_copy(
                src_ref=partial.at[c, owner], dst_ref=returned.at[c, ep],
                send_sem=ret_send.at[c, off], recv_sem=ret_recv.at[c, ep],
                device_id={"ep": owner}, device_id_type=MESH)
            copy.start()
            sends.append(copy)
        returned[c, ep] = partial[c, ep]

    for c in range(chunks):
        for off in range(1, ep_count):
            source = lax.rem(ep + off, ep_count)
            pltpu.make_async_remote_copy(
                src_ref=partial.at[c, source], dst_ref=returned.at[c, source],
                send_sem=ret_send.at[c, off], recv_sem=ret_recv.at[c, source],
                device_id={"ep": source}, device_id_type=MESH).wait_recv()
        for h in range(hid_count):
            block = returned[c, :, :, h * step:(h + 1) * step].reshape(ep_count * cap, step)
            owner_out[c, h] = jnp.dot(combine[...], block, preferred_element_type=F32).astype(BF16)
        for off in list(range(2, hid_count)) + [1]:
            target = lax.rem(hid + off, hid_count)
            copy = pltpu.make_async_remote_copy(
                src_ref=owner_out.at[c, target], dst_ref=owner_in.at[c, hid],
                send_sem=sum_send.at[c, off], recv_sem=sum_recv.at[c, hid],
                device_id={"hid": target}, device_id_type=MESH)
            copy.start()
            sends.append(copy)

    for c in range(chunks):
        total = owner_out[c, hid].astype(F32)
        for off in range(1, hid_count):
            source = lax.rem(hid + off, hid_count)
            pltpu.make_async_remote_copy(
                src_ref=owner_out.at[c, source], dst_ref=owner_in.at[c, source],
                send_sem=sum_send.at[c, off], recv_sem=sum_recv.at[c, source],
                device_id={"hid": source}, device_id_type=MESH).wait_recv()
            total = total + owner_in[c, source].astype(F32)
        out[:, c * step:(c + 1) * step] = total.astype(BF16)
    for copy in sends + forwards:
        copy.wait_send()


def local(ep_count, hid_count, tokens, expert_ids, gate_probs, w_gate, w_up, w_down):
    rows, width = tokens.shape
    inner = w_gate.shape[2]
    cap = rows // 2
    feat = width // hid_count
    step = RETURN_STEP
    chunks = feat // step
    others = max(ep_count // 2 - 1, 1)
    vmem = pl.BlockSpec(memory_space=pltpu.VMEM)
    hbm = pl.BlockSpec(memory_space=pl.ANY)
    dma = pltpu.SemaphoreType.DMA
    return pl.pallas_call(
        functools.partial(kernel, ep_count, hid_count),
        out_shape=jax.ShapeDtypeStruct((rows, feat), BF16),
        in_specs=[vmem, vmem, vmem, hbm, hbm, hbm],
        out_specs=vmem,
        scratch_shapes=[
            pltpu.VMEM((width, inner), BF16),
            pltpu.VMEM((width, inner), BF16),
            pltpu.VMEM((inner, width), BF16),
            pltpu.VMEM((128, rows), jnp.int32),
            pltpu.VMEM((rows, ep_count * cap), BF16),
            pltpu.VMEM((others, 2, cap, width // 2), BF16),
            pltpu.VMEM((cap, width), BF16),
            pltpu.VMEM((ep_count, cap, width), BF16),
            pltpu.VMEM((ep_count * cap, inner), BF16),
            pltpu.VMEM((chunks, ep_count, cap, hid_count * step), BF16),
            pltpu.VMEM((chunks, ep_count, cap, hid_count * step), BF16),
            pltpu.VMEM((chunks, hid_count, rows, step), BF16),
            pltpu.VMEM((chunks, hid_count, rows, step), BF16),
            dma((3,)),
            dma((ep_count // 2, ROW_CHUNKS, 2)),
            dma((ep_count, ROW_CHUNKS)),
            dma((ep_count // 2, ROW_CHUNKS, 2)),
            dma((ep_count // 2, ROW_CHUNKS, 2)),
            dma((chunks, ep_count)),
            dma((chunks, ep_count)),
            dma((chunks, hid_count)),
            dma((chunks, hid_count)),
        ],
        compiler_params=pltpu.CompilerParams(
            collective_id=0, has_side_effects=True, vmem_limit_bytes=60 * 2**20),
    )(tokens, expert_ids.T, gate_probs.T, w_gate, w_up, w_down)


def solution(mesh):
    in_specs = (
        P(("grp", "ep"), None),
        P(("grp", "ep"), None),
        P(("grp", "ep"), None),
        P(("ep", "hid"), None, None),
        P(("ep", "hid"), None, None),
        P(("ep", "hid"), None, None),
    )
    out_specs = P(("grp", "ep"), "hid")
    body = functools.partial(local, mesh.shape["ep"], mesh.shape["hid"])
    return jax.shard_map(body, mesh=mesh, in_specs=in_specs, out_specs=out_specs, check_vma=False)
```

```python
import functools

import jax
import jax.numpy as jnp
from jax import lax
from jax.experimental import pallas as pl
from jax.experimental.pallas import tpu as pltpu
from jax.sharding import PartitionSpec as P

QUARTERS = 4
ROW_CHUNKS = 4
RETURN_STEP = 128
MESH = pl.DeviceIdType.MESH
F32 = jnp.float32
BF16 = jnp.bfloat16


def kernel(ep_count, hid_count, tokens, ids, probs, w_gate, w_up, w_down, out,
           gate_buf, up_buf, down_buf, key_t, combine, outgoing, sibling_out, slots, hidden,
           partial, returned, owner_out, owner_in,
           weight_sem, disp_send, disp_recv, fwd_send, fwd_recv, ret_send, ret_recv, sum_send, sum_recv):
    ep = lax.axis_index("ep")
    hid = lax.axis_index("hid")
    groups = hid_count // QUARTERS
    group = hid // QUARTERS
    rows, width = tokens.shape
    picks = ids.shape[0]
    cap = slots.shape[1]
    half = width // 2
    pairs = ep_count // 2
    pair = ep // 2
    core = ep % 2
    sibling = pair * 2 + 1 - core
    mate = hid + 1 - 2 * (hid % 2)
    my_half = pl.ds(pl.multiple_of((hid % 2) * half, half), half)
    piece = cap // ROW_CHUNKS
    feat = width // hid_count
    chunks = partial.shape[0]
    inner = gate_buf.shape[1]
    row_groups = ((0, 1), (1, ROW_CHUNKS)) if pairs == 2 else ((0, ROW_CHUNKS),)
    step = feat // chunks

    loads = [pltpu.make_async_copy(src.at[0], dst, weight_sem.at[i])
             for i, (src, dst) in enumerate(((w_gate, gate_buf), (w_up, up_buf), (w_down, down_buf)))]
    for load in loads:
        load.start()

    barrier = pltpu.get_barrier_semaphore()
    for off in range(1, ep_count):
        pl.semaphore_signal(barrier, 1, device_id={"ep": lax.rem(ep + off, ep_count)}, device_id_type=MESH)
    for off in range(1, hid_count):
        pl.semaphore_signal(barrier, 1, device_id={"hid": lax.rem(hid + off, hid_count)}, device_id_type=MESH)

    name = lax.broadcasted_iota(jnp.int32, (128, rows), 0) * groups + group
    count = jnp.zeros((128, rows), F32)
    weight = jnp.zeros((128, rows), F32)
    gate_round = probs[...].astype(BF16).astype(F32)
    for k in range(picks):
        hit = ids[k:k + 1, :] == name
        count = jnp.where(hit, 1.0, count)
        weight = jnp.where(hit, gate_round[k:k + 1, :], weight)
    earlier = (lax.broadcasted_iota(jnp.int32, (rows, rows), 0)
               < lax.broadcasted_iota(jnp.int32, (rows, rows), 1)).astype(F32).astype(BF16)
    before = jnp.dot(count.astype(BF16), earlier, preferred_element_type=F32)
    place = jnp.where(count > 0.5, before, -1000.0)
    key_t[...] = place.astype(jnp.int32)

    def pick_rows(first, blocks):
        row = lax.broadcasted_iota(jnp.int32, (cap, rows), 0)
        parts = [(key_t[pl.ds(first + b, 1), :] == row).astype(F32).astype(BF16) for b in range(blocks)]
        return jnp.concatenate(parts, axis=0) if blocks > 1 else parts[0]

    tile = min(half, 512)
    sends = []
    for off in range(1, pairs):
        other = lax.rem(pair + off, pairs)
        chosen = pick_rows(2 * other, 2)
        for col in range(0, half, tile):
            src = pl.ds(pl.multiple_of((hid % 2) * half + col, tile), tile)
            rows_out = jnp.dot(chosen, tokens[:, src], preferred_element_type=F32).astype(BF16)
            outgoing[off - 1, :, :, col:col + tile] = rows_out.reshape(2, cap, tile)
    pl.semaphore_wait(barrier, ep_count - 1 + hid_count - 1)
    for off in range(1, pairs):
        other = lax.rem(pair + off, pairs)
        for r in range(ROW_CHUNKS):
            part = pl.ds(r * piece, piece)
            for flip in range(2):
                who = core if flip == 0 else 1 - core
                copy = pltpu.make_async_remote_copy(
                    src_ref=outgoing.at[off - 1, who, part],
                    dst_ref=slots.at[ep, part, my_half],
                    send_sem=disp_send.at[off, r, flip],
                    recv_sem=disp_recv.at[ep, r],
                    device_id={"ep": 2 * other + who}, device_id_type=MESH)
                copy.start()
                sends.append(copy)

    for col in range(0, width, tile):
        sibling_out[:, col:col + tile] = jnp.dot(
            pick_rows(sibling, 1), tokens[:, col:col + tile], preferred_element_type=F32).astype(BF16)
    to_sibling = pltpu.make_async_remote_copy(
        src_ref=sibling_out, dst_ref=slots.at[ep],
        send_sem=disp_send.at[0, 0, 0], recv_sem=disp_recv.at[ep, 0],
        device_id={"ep": sibling}, device_id_type=MESH)
    to_sibling.start()
    sends.append(to_sibling)
    for col in range(0, width, tile):
        slots[ep, :, col:col + tile] = jnp.dot(
            pick_rows(ep, 1), tokens[:, col:col + tile], preferred_element_type=F32).astype(BF16)

    lanes = lax.broadcasted_iota(jnp.int32, (rows, cap), 1)
    key = place.T.astype(jnp.int32)
    weight = weight.T
    for b in range(ep_count):
        combine[:, b * cap:(b + 1) * cap] = jnp.where(
            key[:, b:b + 1] == lanes, weight[:, b:b + 1], 0.0).astype(BF16)

    def act(which, start, size):
        block = slots[pl.ds(2 * which, 2), start:start + size].reshape(2 * size, width)
        gate_act = jnp.dot(block, gate_buf[...], preferred_element_type=F32)
        up_act = jnp.dot(block, up_buf[...], preferred_element_type=F32)
        value = gate_act / (1.0 + jnp.exp(-gate_act)) * up_act
        hidden[pl.ds(2 * which, 2), start:start + size] = value.astype(BF16).reshape(2, size, inner)

    def down(first, pair_count, start, size, c):
        block = hidden[pl.ds(2 * first, 2 * pair_count), start:start + size]
        block = block.reshape(2 * pair_count * size, inner)
        for h in range(hid_count):
            col = h * feat + c * step
            value = jnp.dot(block, down_buf[:, col:col + step], preferred_element_type=F32)
            partial[c, pl.ds(2 * first, 2 * pair_count), start:start + size, h * step:(h + 1) * step] = (
                value.astype(BF16).reshape(2 * pair_count, size, step))

    def give_back(owner, start, size, c, g):
        return pltpu.make_async_remote_copy(
            src_ref=partial.at[c, owner, pl.ds(start, size)],
            dst_ref=returned.at[c, ep, pl.ds(start, size)],
            send_sem=ret_send.at[c, owner, g], recv_sem=ret_recv.at[c, ep, g],
            device_id={"ep": owner}, device_id_type=MESH)

    def take_back(source, start, size, c, g):
        landed = returned.at[c, source, pl.ds(start, size)]
        pltpu.make_async_remote_copy(
            src_ref=landed, dst_ref=landed,
            send_sem=ret_send.at[c, source, g], recv_sem=ret_recv.at[c, source, g],
            device_id={"ep": source}, device_id_type=MESH).wait_recv()

    pltpu.make_async_remote_copy(
        src_ref=sibling_out, dst_ref=slots.at[sibling],
        send_sem=disp_send.at[0, 0, 0], recv_sem=disp_recv.at[sibling, 0],
        device_id={"ep": sibling}, device_id_type=MESH).wait_recv()
    loads[0].wait()
    loads[1].wait()
    act(pair, 0, cap)

    forwards = {}

    def forward(r):
        part = pl.ds(r * piece, piece)
        for off in range(1, pairs):
            other = lax.rem(pair + pairs - off, pairs)
            for flip in range(2):
                source = 2 * other + (core if flip == 0 else 1 - core)
                landed = slots.at[source, part, my_half]
                pltpu.make_async_remote_copy(
                    src_ref=landed, dst_ref=landed,
                    send_sem=disp_send.at[off, r, flip], recv_sem=disp_recv.at[source, r],
                    device_id={"ep": source}, device_id_type=MESH).wait_recv()
                copy = pltpu.make_async_remote_copy(
                    src_ref=landed, dst_ref=landed,
                    send_sem=fwd_send.at[off, r, flip], recv_sem=fwd_recv.at[off, r, flip],
                    device_id={"hid": mate}, device_id_type=MESH)
                copy.start()
                forwards[off, r, flip] = copy

    loads[2].wait()
    passed = 0
    for g, (low, high) in enumerate(row_groups):
        start, size = low * piece, (high - low) * piece
        last = g == len(row_groups) - 1
        for r in range(passed, ROW_CHUNKS if last else high + 1):
            forward(r)
        passed = high + 1
        for off in range(1, pairs):
            for r in range(low, high):
                for flip in range(2):
                    forwards[off, r, flip].wait_recv()
            act(lax.rem(pair + pairs - off, pairs), start, size)
        for c in range(chunks):
            if len(row_groups) > 1:
                down(1 - pair, 1, start, size, c)
            else:
                down(0, pairs, 0, cap, c)
            for off in range(1, pairs):
                other = lax.rem(pair + off, pairs)
                for who in (core, 1 - core):
                    copy = give_back(2 * other + who, start, size, c, g)
                    copy.start()
                    sends.append(copy)
            if last:
                if len(row_groups) > 1:
                    down(pair, 1, 0, cap, c)
                copy = give_back(sibling, 0, cap, c, 0)
                copy.start()
                sends.append(copy)
                returned[c, ep] = partial[c, ep]

    for c in range(chunks):
        take_back(sibling, 0, cap, c, 0)
        for off in range(1, pairs):
            other = lax.rem(pair + pairs - off, pairs)
            for who in (core, 1 - core):
                for g, (low, high) in enumerate(row_groups):
                    take_back(2 * other + who, low * piece, (high - low) * piece, c, g)
        for h in range(hid_count):
            block = returned[c, :, :, h * step:(h + 1) * step].reshape(ep_count * cap, step)
            owner_out[c, h] = jnp.dot(combine[...], block, preferred_element_type=F32).astype(BF16)
        for off in list(range(2, hid_count)) + [1]:
            target = lax.rem(hid + off, hid_count)
            copy = pltpu.make_async_remote_copy(
                src_ref=owner_out.at[c, target], dst_ref=owner_in.at[c, hid],
                send_sem=sum_send.at[c, off], recv_sem=sum_recv.at[c, hid],
                device_id={"hid": target}, device_id_type=MESH)
            copy.start()
            sends.append(copy)

    for c in range(chunks):
        total = owner_out[c, hid].astype(F32)
        for off in range(1, hid_count):
            source = lax.rem(hid + off, hid_count)
            pltpu.make_async_remote_copy(
                src_ref=owner_out.at[c, source], dst_ref=owner_in.at[c, source],
                send_sem=sum_send.at[c, off], recv_sem=sum_recv.at[c, source],
                device_id={"hid": source}, device_id_type=MESH).wait_recv()
            total = total + owner_in[c, source].astype(F32)
        out[:, c * step:(c + 1) * step] = total.astype(BF16)
    for copy in sends + list(forwards.values()):
        copy.wait_send()


def local(ep_count, hid_count, tokens, expert_ids, gate_probs, w_gate, w_up, w_down):
    rows, width = tokens.shape
    inner = w_gate.shape[2]
    cap = rows // 2
    feat = width // hid_count
    step = RETURN_STEP
    chunks = feat // step
    others = max(ep_count // 2 - 1, 1)
    vmem = pl.BlockSpec(memory_space=pltpu.VMEM)
    hbm = pl.BlockSpec(memory_space=pl.ANY)
    dma = pltpu.SemaphoreType.DMA
    return pl.pallas_call(
        functools.partial(kernel, ep_count, hid_count),
        out_shape=jax.ShapeDtypeStruct((rows, feat), BF16),
        in_specs=[vmem, vmem, vmem, hbm, hbm, hbm],
        out_specs=vmem,
        scratch_shapes=[
            pltpu.VMEM((width, inner), BF16),
            pltpu.VMEM((width, inner), BF16),
            pltpu.VMEM((inner, width), BF16),
            pltpu.VMEM((128, rows), jnp.int32),
            pltpu.VMEM((rows, ep_count * cap), BF16),
            pltpu.VMEM((others, 2, cap, width // 2), BF16),
            pltpu.VMEM((cap, width), BF16),
            pltpu.VMEM((ep_count, cap, width), BF16),
            pltpu.VMEM((ep_count, cap, inner), BF16),
            pltpu.VMEM((chunks, ep_count, cap, hid_count * step), BF16),
            pltpu.VMEM((chunks, ep_count, cap, hid_count * step), BF16),
            pltpu.VMEM((chunks, hid_count, rows, step), BF16),
            pltpu.VMEM((chunks, hid_count, rows, step), BF16),
            dma((3,)),
            dma((ep_count // 2, ROW_CHUNKS, 2)),
            dma((ep_count, ROW_CHUNKS)),
            dma((ep_count // 2, ROW_CHUNKS, 2)),
            dma((ep_count // 2, ROW_CHUNKS, 2)),
            dma((chunks, ep_count, 2)),
            dma((chunks, ep_count, 2)),
            dma((chunks, hid_count)),
            dma((chunks, hid_count)),
        ],
        compiler_params=pltpu.CompilerParams(
            collective_id=0, has_side_effects=True, vmem_limit_bytes=60 * 2**20),
    )(tokens, expert_ids.T, gate_probs.T, w_gate, w_up, w_down)


def solution(mesh):
    in_specs = (
        P(("grp", "ep"), None),
        P(("grp", "ep"), None),
        P(("grp", "ep"), None),
        P(("ep", "hid"), None, None),
        P(("ep", "hid"), None, None),
        P(("ep", "hid"), None, None),
    )
    out_specs = P(("grp", "ep"), "hid")
    body = functools.partial(local, mesh.shape["ep"], mesh.shape["hid"])
    return jax.shard_map(body, mesh=mesh, in_specs=in_specs, out_specs=out_specs, check_vma=False)
```
